128 devices in a mesh: ep: 32 (over x, z, core), etp: 4 (over y).
Axes of the slice: x: 4, y: 4, z: 4, core: 2. Of those that a mesh axis runs over, the one named last changes fastest.
Arguments:
- tokens: bfloat16 [4096, 4096], P('ep', 'etp'), may hold values from -6 to 6
- expert_ids: int32 [4096, 8], P('ep'), may hold values from 0 to 63, all different within a row; in each aligned block of 128 rows (0 to 127, 128 to 255, ...) at most 24 rows name the same one
- gate_prob: float32 [4096, 8], P('ep'), may hold values from 0.05 to 1
- gate_weight: bfloat16 [64, 4096, 1536], P('ep', None, 'etp'), may hold values from -0.09375 to 0.09375
- up_weight: bfloat16 [64, 4096, 1536], P('ep', None, 'etp'), may hold values from -0.09375 to 0.09375
- down_weight: bfloat16 [64, 1536, 4096], P('ep', 'etp'), may hold values from -0.15625 to 0.15625
Outputs:
- mixed: bfloat16 [4096, 4096], P('ep', 'etp')
The draws below stay inside these ranges and needn't reach their ends.
Inputs may be any that keep to these rules, and one draw needn't show every extreme that they name: `expert_ids`: each row names 8 different experts. Within each aligned block of 128 rows (one token group) no expert is named more than 24 times, and in every draw some expert is named exactly 24 times in some block.
All inputs are finite; a program needn't handle non-finite values.
Results may differ from the reference program's by a relative error of at most 0.012.
Values may be sent and summed in bfloat16 or wider, within the bound.
No kernel may reach another device: no remote copies, remote signals or barrier semaphores. Data moves between devices by JAX's collectives and lax.ppermute only.
A program may use at most 128 MiB of HBM per device.

```python
import math
import jax
import jax.numpy as jnp
import numpy as np
from jax import lax

D = 4096
FF = 1536
TOP = 8
TOK_DEV = 128
EXPERTS = 64
GROUPS = 32
TOKENS = 4096
CAP = 24
N_ETP = 4


def shard_levels(rng, shape, split, least, top_value):
    level, own = 1.0, jax.random.fold_in(rng, 6)
    for dim, shards_of in split:
        draws = jnp.exp(jax.random.uniform(jax.random.fold_in(own, dim), (shards_of,), jnp.float32, least / len(split), top_value / len(split)))
        level = level * jnp.repeat(draws, shape[dim] // shards_of).reshape([-1 if axis == dim else 1 for axis in range(len(shape))])
    return level


def assign_block(stream_key, own, number, rows, count, top, most, lean):
    ranking = jax.random.permutation(stream_key, count)
    packed, ordinary = load_shares(count, rows * top, most, lean, True), load_shares(count, rows * top, most, lean, False)
    places = jnp.arange(count)

    def named(lengths, offset_by):
        used = int((lengths > 0).sum())
        fixed = max(1, used // 4)
        moved = fixed + (places - fixed + offset_by * (used - fixed)) % max(1, count - fixed)
        return jnp.zeros((count,), jnp.int32).at[ranking[jnp.where(places < fixed, places, moved)]].set(jnp.asarray(lengths, jnp.int32))

    lengths = jnp.where(number % 4 == 0, named(packed, number // 4), named(ordinary, number - number // 4 - 1))
    mixed = jax.random.permutation(jax.random.fold_in(own, 3), count)
    source_of, sink = mixed[0:count // 2 * 2:2], mixed[1:count // 2 * 2:2]
    slack = jnp.minimum(lengths[source_of] - 1, most - lengths[sink]) // 2
    slack = jnp.where((source_of == ranking[0]) | (sink == ranking[0]) | (lengths[sink] == 0), 0, jnp.maximum(slack, 0))
    moved = jax.random.randint(jax.random.fold_in(own, 4), (count // 2,), 0, 1 << 20) % (slack + 1)
    lengths = lengths.at[source_of].add(-moved).at[sink].add(moved)
    items = jnp.searchsorted(jnp.cumsum(lengths), jnp.arange(rows * top), side="right").astype(jnp.int32)
    grid = items.reshape(top, rows).T
    grid = grid[jax.random.permutation(jax.random.fold_in(own, 1), rows)]
    offset_by = jax.random.randint(jax.random.fold_in(own, 2), (rows, 1), 0, top)
    return jnp.take_along_axis(grid, (jnp.arange(top)[None, :] + offset_by) % top, axis=1)


def load_shares(amount, total, limit, slope, full):
    weights = [(1 << 20) // math.isqrt(standing ** slope) + 1 for standing in range(1, amount + 1)]
    largest = limit if full else min(limit, max(-(-total // amount), total * weights[0] // sum(weights)))
    least = 1 if total - largest >= amount - 1 else 0
    given, rest = [largest] + [least] * (amount - 1), total - largest - least * (amount - 1)
    while rest > 0:
        free = [i for i in range(1, amount) if given[i] < largest] or [i for i in range(1, amount) if given[i] < limit]
        whole, remaining = sum([weights[i] for i in free]), rest
        for i in free:
            more = min(limit - given[i], max(1, remaining * weights[i] // whole), rest)
            given[i] = given[i] + more
            rest = rest - more
    return np.array(given)


def scatter_about(own_key, dims, spread, most, pieces=(), kind=jnp.bfloat16):
    result = jax.random.normal(own_key, dims, jnp.float32) * spread
    if len(pieces) > 0:
        result = shard_levels(own_key, dims, pieces, -0.22, 0.18) * result
    return jnp.clip(result, min=-most, max=most).astype(kind)


def setup_inputs(seed: int = 0) -> dict:
    splits = jax.random.split(jax.random.key(seed), 7)
    tokens = scatter_about(splits[0], (TOKENS, D), 1.0, 6.0, ((0, 32), (1, 4)))
    expert_ids_keys = jax.random.split(jax.random.fold_in(splits[1], 1), TOKENS // TOK_DEV)
    expert_ids_turns = jax.random.permutation(jax.random.fold_in(splits[1], 3), TOKENS // TOK_DEV)
    expert_ids = jax.vmap(lambda own, number: assign_block(jax.random.fold_in(splits[1], 2), own, number, TOK_DEV, EXPERTS, TOP, CAP, 2))(expert_ids_keys, expert_ids_turns).reshape((TOKENS, TOP))
    gate_prob = jnp.clip(0.05 + 0.95 * jax.random.uniform(splits[2], (TOKENS, TOP), jnp.float32) ** shard_levels(splits[2], (TOKENS, TOP), ((0, 32),), -0.2, 0.2), 0.05, 1.0)
    gate_weight = scatter_about(splits[3], (EXPERTS, D, FF), D ** -0.5, 0.09375, ((0, 32), (2, 4)))
    up_weight = scatter_about(splits[4], (EXPERTS, D, FF), D ** -0.5, 0.09375, ((0, 32), (2, 4)))
    down_weight = scatter_about(splits[5], (EXPERTS, FF, D), FF ** -0.5, 0.15625, ((0, 32), (1, 4)))
    return dict(tokens=tokens, expert_ids=expert_ids, gate_prob=gate_prob, gate_weight=gate_weight, up_weight=up_weight, down_weight=down_weight)


def reference(tokens, expert_ids, gate_prob, gate_weight, up_weight, down_weight):
    assigned = TOK_DEV * TOP
    grouped = expert_ids.reshape(GROUPS, assigned).astype(jnp.int32)
    onehot = (grouped[:, :, None] == jnp.arange(EXPERTS, dtype=jnp.int32)[None, None, :]).astype(jnp.int32)
    position = jnp.sum((jnp.cumsum(onehot, axis=1) - onehot) * onehot, axis=2).astype(jnp.int32)
    slot_index = (grouped * CAP + position).astype(jnp.int32)
    group_rows = jnp.arange(GROUPS, dtype=jnp.int32)[:, None]
    owners = (group_rows * TOK_DEV + (jnp.arange(assigned, dtype=jnp.int32) // TOP)[None, :]).astype(jnp.int32)
    sources = jnp.full((GROUPS, EXPERTS * CAP), TOKENS, jnp.int32).at[group_rows, slot_index].set(owners)
    scales = jnp.zeros((GROUPS, EXPERTS * CAP), jnp.float32).at[group_rows, slot_index].set(
        gate_prob.reshape(GROUPS, assigned).astype(jnp.float32))
    sources = sources.reshape(GROUPS, EXPERTS, CAP).transpose(1, 0, 2).reshape(EXPERTS, GROUPS * CAP)
    scales = scales.reshape(GROUPS, EXPERTS, CAP).transpose(1, 0, 2).reshape(EXPERTS, GROUPS * CAP)
    padded = jnp.concatenate([tokens, jnp.zeros((1, D), tokens.dtype)], axis=0)
    block = FF // N_ETP

    def expert_step(accumulated, inputs):
        w_gate, w_up, w_down, rows_from, row_scale = inputs
        expert_rows = padded[rows_from]
        gate_sum = jnp.dot(expert_rows, w_gate, preferred_element_type=jnp.float32)
        up_sum = jnp.dot(expert_rows, w_up, preferred_element_type=jnp.float32)
        hidden = (jax.nn.silu(gate_sum) * up_sum).astype(jnp.bfloat16)
        expert_out = jnp.zeros((GROUPS * CAP, D), jnp.float32)
        for part_index in range(N_ETP):
            product = jnp.dot(hidden[:, part_index * block:(part_index + 1) * block],
                              w_down[part_index * block:(part_index + 1) * block, :],
                              preferred_element_type=jnp.float32)
            rounded = lax.optimization_barrier(product.astype(jnp.bfloat16))
            expert_out = expert_out + rounded.astype(jnp.float32)
        accumulated = accumulated.at[rows_from].add(row_scale[:, None] * expert_out)
        return accumulated, None

    accumulated = jnp.zeros((TOKENS + 1, D), jnp.float32)
    accumulated, unused = lax.scan(expert_step, accumulated,
                                   (gate_weight, up_weight, down_weight, sources, scales))
    return accumulated[:TOKENS].astype(jnp.bfloat16)
```

```python
import jax
import jax.numpy as jnp
from jax import lax
from jax.experimental import pallas as pl
from jax.experimental.pallas import tpu as pltpu
from jax.sharding import PartitionSpec as P


SIDE = 4
CAP = 24
TOK = 128
FA, FB, FC = 384, 384, 256
B_ORDER = (0, 2, 1, 3)
BF = jnp.bfloat16
F32 = jnp.float32
VMEM = 60 * 1024 * 1024


def ep_of(x, z, c):
    return ((x % SIDE) * SIDE + z % SIDE) * 2 + c


def recv(a, dim, d):
    if dim == "y":
        return lax.ppermute(a, "etp", [((i + d) % SIDE, i) for i in range(SIDE)])
    dx, dz, flip = (d, 0, 0) if dim == "x" else (0, d, 0) if dim == "z" else (0, 0, 1)
    pairs = [(ep_of(x + dx, z + dz, c ^ flip), ep_of(x, z, c))
             for x in range(SIDE) for z in range(SIDE) for c in range(2)]
    return lax.ppermute(a, "ep", pairs)


def gather_direct(a, dim):
    return [a] + [recv(a, dim, d) for d in (1, 2, 3)]


def gather_ring(h0, h1, dim):
    r10 = recv(h0, dim, 1)
    r31 = recv(h1, dim, -1)
    r11 = recv(h1, dim, 1)
    r30 = recv(h0, dim, -1)
    r20 = recv(r10, dim, 1)
    r21 = recv(r31, dim, -1)
    return [(h0, h1), (r10, r11), (r20, r21), (r30, r31)]


def add(*terms):
    total = terms[0].astype(F32)
    for t in terms[1:]:
        total = total + t.astype(F32)
    return total


def scatter_ring(blocks, dim):
    (b00, b01), (b10, b11), (b20, b21), (b30, b31) = blocks
    s0 = recv(b20, dim, -1)
    s1 = recv(b21, dim, 1)
    i1 = recv(b11, dim, -1)
    j0 = recv(b30, dim, 1)
    i0 = recv(add(b10, s0).astype(BF), dim, -1)
    j1 = recv(add(b31, s1).astype(BF), dim, 1)
    return add(b00, i0, j0).astype(BF), add(b01, i1, j1).astype(BF)


def scatter_direct(blocks, dim):
    return add(blocks[0], *[recv(blocks[d], dim, -d) for d in (1, 2, 3)])


def dot(a, b):
    return jnp.dot(a, b, preferred_element_type=F32)


def spec(shape, index):
    return pl.BlockSpec(shape, index)


def call(kernel, grid, in_specs, out_specs, out_shapes, name, scratch=(), **kw):
    return pl.pallas_call(
        kernel, grid=grid, in_specs=in_specs, out_specs=out_specs,
        out_shape=[jax.ShapeDtypeStruct(s, BF) for s in out_shapes],
        scratch_shapes=scratch, name=name,
        compiler_params=pltpu.CompilerParams(vmem_limit_bytes=VMEM, dimension_semantics=("arbitrary",) * len(grid)), **kw)


def put_rows(own, par, rows, at, col, width):
    for e in range(2):
        own[e, at:at + 48, col:col + width] = rows[e * 48:(e + 1) * 48].astype(BF)
        par[e, at:at + 48, col:col + width] = rows[(e + 2) * 48:(e + 3) * 48].astype(BF)


def select_a_body(p, *refs):
    xs, (own, par) = refs[:8], refs[8:]
    for k in range(8):
        put_rows(own, par, dot(p[k], xs[k][0].reshape(2 * TOK, FA)), k * 48, 0, FA)


def select_b_body(p, *refs):
    xs, (own, par) = refs[:8], refs[8:]
    for d in range(4):
        for h in range(2):
            for q in range(2):
                x = xs[d * 2 + h][2 * q:2 * q + 2, 0].reshape(2 * TOK, FB)
                put_rows(own, par, dot(p[d * 2 + q], x), (d * 2 + q) * 48, h * FB, FB)


def select_c_body(p, *refs):
    xs, (own, par) = refs[:8], refs[8:]
    for d in range(4):
        for h in range(2):
            put_rows(own, par, dot(p[h], xs[d * 2 + h][0].reshape(2 * TOK, FC)), h * 48, d * FC, FC)


FULL_P = spec((8, 192, 256), lambda i: (0, 0, 0))
HALF_P = spec((2, 192, 256), lambda i: (i, 0, 0))
A_BLOCK = spec((1, 2, TOK, FA), lambda i: (i, 0, 0, 0))
B_BLOCK = spec((4, 1, TOK, FB), lambda i: (0, i, 0, 0))
C_BLOCK = spec((1, 2, TOK, FC), lambda i: (i, 0, 0, 0))
A_ROWS = spec((2, 384, FA), lambda i: (0, 0, i))
B_ROWS = spec((2, 384, 2 * FB), lambda i: (0, 0, i))
C_ROWS = spec((2, 96, 4 * FC), lambda i: (0, i, 0))
ROWS_A, ROWS_B, ROWS_C = (2, 384, 4 * FA), (2, 384, 4 * FB), (2, 384, 4 * FC)


def select(piece, p, blocks):
    flat = [half for pair in blocks for half in pair]
    body, n, pspec, xspec, rspec, rshape = {
        "a": (select_a_body, 4, FULL_P, A_BLOCK, A_ROWS, ROWS_A),
        "b": (select_b_body, 2, FULL_P, B_BLOCK, B_ROWS, ROWS_B),
        "c": (select_c_body, 4, HALF_P, C_BLOCK, C_ROWS, ROWS_C)}[piece]
    return call(body, (n,), [pspec] + [xspec] * 8, [rspec] * 2, [rshape] * 2, "select_" + piece)(p, *flat)


def pick(own, rcv, at):
    return jnp.concatenate([r[e, at:at + 48, :] for r in (own, rcv) for e in range(2)], axis=0)


def tdot(p, rows):
    return lax.dot_general(p, rows, (((0,), (0,)), ((), ())), preferred_element_type=F32).astype(BF)


def combine_a_body(p, own, rcv, *outs):
    for k in range(8):
        outs[k][0] = tdot(p[k], pick(own, rcv, k * 48)).reshape(2, TOK, FA)


def combine_b_body(p, own, rcv, *outs):
    for d in range(4):
        for q in range(2):
            r = tdot(p[d * 2 + q], pick(own, rcv, (d * 2 + q) * 48))
            for h in range(2):
                outs[d * 2 + h][2 * q:2 * q + 2, 0] = r[:, h * FB:(h + 1) * FB].reshape(2, TOK, FB)


def combine_c_body(p, own, rcv, *outs):
    for h in range(2):
        r = tdot(p[h], pick(own, rcv, h * 48))
        for d in range(4):
            outs[d * 2 + h][0] = r[:, d * FC:(d + 1) * FC].reshape(2, TOK, FC)


def combine(piece, p, own, rcv):
    body, n, pspec, ospec, rspec, oshape = {
        "a": (combine_a_body, 4, FULL_P, A_BLOCK, A_ROWS, (4, 2, TOK, FA)),
        "b": (combine_b_body, 2, FULL_P, B_BLOCK, B_ROWS, (4, 2, TOK, FB)),
        "c": (combine_c_body, 4, HALF_P, C_BLOCK, C_ROWS, (4, 2, TOK, FC))}[piece]
    o = call(body, (n,), [pspec, rspec, rspec], [ospec] * 8, [oshape] * 8, "combine_" + piece)(p, own, rcv)
    return [(o[2 * d], o[2 * d + 1]) for d in range(4)]


def weight_copies(y, e, wg, wu, wd, gu, dn, sems):
    copies = []
    n = 0
    for base, width, order, at in ((0, FA, (0, 1, 2, 3), 0), (FA, FB, B_ORDER, 4 * FA), (FA + FB, FC, (0, 1, 2, 3), 4 * (FA + FB))):
        for k, dy in enumerate(order):
            src = pl.ds(pl.multiple_of(lax.rem(y + dy, SIDE) * 1024 + base, 128), width)
            dst = pl.ds(at + k * width, width)
            copies.append(pltpu.make_async_copy(wg.at[e, src, :], gu.at[e, dst, pl.ds(0, 384)], sems.at[e, n]))
            copies.append(pltpu.make_async_copy(wu.at[e, src, :], gu.at[e, dst, pl.ds(384, 384)], sems.at[e, n + 1]))
            copies.append(pltpu.make_async_copy(wd.at[e, :, src], dn.at[e, :, dst], sems.at[e, n + 2]))
            n += 3
    return copies


def experts_body(y_ref, a0, b0, c0, a1, b1, c1, wg, wu, wd, oa0, ob0, oc0, oa1, ob1, oc1, gu, dn, first, acc, hs, sems):
    e = pl.program_id(0)
    y = y_ref[0]

    @pl.when(e == 0)
    def _():
        for k in range(2):
            for cp in weight_copies(y, k, wg, wu, wd, gu, dn, sems):
                cp.start()

    for k in range(2):
        @pl.when(e == k)
        def _(k=k):
            for cp in weight_copies(y, k, wg, wu, wd, gu, dn, sems):
                cp.wait()

    for half, (a, b, c, oa, ob, oc) in enumerate(((a0, b0, c0, oa0, ob0, oc0), (a1, b1, c1, oa1, ob1, oc1))):
        first[...] = dot(a[0], gu[e, 0:4 * FA, :])
        acc[...] = dot(b[0], gu[e, 4 * FA:4 * (FA + FB), :])
        acc[...] += dot(c[0], gu[e, 4 * (FA + FB):4096, :])
        for i in range(4):
            for j in range(4):
                to, fro = (i * 4 + j) * CAP, (j * 4 + i) * CAP
                v = acc[to:to + CAP, :] + first[fro:fro + CAP, :]
                g, u = v[:, :384], v[:, 384:]
                hs[to:to + CAP, :] = g * (1.0 / (1.0 + jnp.exp(-g))) * u
        h2 = hs[...].astype(BF)
        h1 = jnp.concatenate([hs[(j * 4 + i) * CAP:(j * 4 + i + 1) * CAP, :] for i in range(4) for j in range(4)], axis=0).astype(BF)
        oa[0] = dot(h1, dn[e, :, 0:4 * FA]).astype(BF)
        ob[0] = dot(h2, dn[e, :, 4 * FA:4 * (FA + FB)]).astype(BF)
        oc[0] = dot(h2, dn[e, :, 4 * (FA + FB):4096]).astype(BF)


def experts(y, own, rcv, wg, wu, wd):
    rows = [spec((1,) + s[1:], lambda e: (e, 0, 0)) for s in (ROWS_A, ROWS_B, ROWS_C)]
    hbm = pl.BlockSpec(memory_space=pl.ANY)
    scratch = [pltpu.VMEM((2, 4096, 768), BF), pltpu.VMEM((2, 384, 4096), BF), pltpu.VMEM((384, 768), F32),
               pltpu.VMEM((384, 768), F32), pltpu.VMEM((384, 384), F32), pltpu.SemaphoreType.DMA((2, 36))]
    o = call(experts_body, (2,), [pl.BlockSpec(memory_space=pltpu.SMEM)] + rows * 2 + [hbm] * 3, rows * 2,
             [ROWS_A, ROWS_B, ROWS_C] * 2, "experts", scratch)(y, *own, *rcv, wg, wu, wd)
    return o[:3], o[3:]


def tables(meta, ep):
    columns = meta.astype(F32).transpose(0, 2, 1)
    ids, prob = columns[:, :8], columns[:, 8:]
    mate = jnp.bitwise_xor(ep, 1)
    named = jnp.stack([2 * ep, 2 * ep + 1, 2 * mate, 2 * mate + 1]).astype(F32)
    hit = ids[:, None, :, :] == named[None, :, None, None]
    match = jnp.any(hit, axis=2)
    weight = jnp.sum(jnp.where(hit, prob[:, None, :, :], 0.0), axis=2)
    t = jnp.arange(TOK)
    before = (t[:, None] < t[None, :]).astype(BF)
    place = jnp.einsum("get,tu->geu", match.astype(BF), before, preferred_element_type=F32)
    place = jnp.where(match, place, -1.0)

    def build(order):
        pl_o = place.reshape(4, 4, 4, TOK).transpose(order).reshape(8, 2, 4, TOK)
        w_o = weight.reshape(4, 4, 4, TOK).transpose(order).reshape(8, 2, 4, TOK)
        r = jnp.arange(CAP, dtype=F32)
        eye = jnp.arange(2)
        on = (pl_o.transpose(0, 2, 1, 3)[:, :, None, None, :, :] == r[None, None, None, :, None, None]) \
            & (eye[:, None] == eye[None, :])[None, None, :, None, :, None]
        sel = on.astype(BF)
        wgt = jnp.where(on, w_o.transpose(0, 2, 1, 3)[:, :, None, None, :, :], 0.0).astype(BF)
        return sel.reshape(8, 192, 256), wgt.reshape(8, 192, 256)

    sel2, wgt2 = build((0, 1, 2, 3))
    sel1, wgt1 = build((1, 0, 2, 3))
    return sel1, wgt1, sel2, wgt2


def body(tokens, expert_ids, gate_prob, gate_weight, up_weight, down_weight):
    ep = lax.axis_index("ep")
    y = lax.axis_index("etp").astype(jnp.int32).reshape(1)
    meta = jnp.concatenate([expert_ids.astype(BF), gate_prob.astype(BF), jnp.zeros((TOK, 112), BF)], axis=1)
    a = tokens[:, :FA]
    b = tokens[:, FA:FA + FB]
    c = jnp.concatenate([tokens[:, FA + FB:], meta], axis=1)

    c4 = gather_direct(c, "z")
    a4 = gather_direct(a, "x")
    b4 = gather_direct(b, "y")
    halves = lambda q: (jnp.stack(q[:2]), jnp.stack(q[2:]))
    c8 = gather_ring(*halves(c4), "x")
    a8 = gather_ring(*halves(a4), "y")
    b8 = gather_ring(*halves(b4), "z")
    ch = [jnp.stack([q[h] for q in c8]) for h in range(2)]
    ah = [jnp.stack([q[h] for q in a8]) for h in range(2)]
    bh = [jnp.stack([q[h] for q in b8]) for h in range(2)]
    xa = gather_ring(*ah, "z")
    xb = gather_ring(*bh, "x")
    xc = gather_ring(*[h[..., :FC] for h in ch], "y")
    info = jnp.stack([h[..., FC:FC + 16] for h in ch], axis=1).reshape(16, TOK, 16)
    sel1, wgt1, sel2, wgt2 = tables(info, ep)

    own, par = zip(select("a", sel1, xa), select("b", sel2, xb), select("c", sel2, xc))
    rcv = [recv(q, "c", 1) for q in par]
    out_own, out_par = experts(y, own, rcv, gate_weight, up_weight, down_weight)
    back = [recv(q, "c", 1) for q in out_par]

    da = combine("a", wgt1, out_own[0], back[0])
    db = combine("b", wgt2, out_own[1], back[1])
    dc = combine("c", wgt2, out_own[2], back[2])
    ra = scatter_ring(da, "z")
    rb = scatter_ring(db, "x")
    rc = scatter_ring(dc, "y")
    rows = lambda r: [(r[0][d], r[1][d]) for d in range(4)]
    ra = scatter_ring(rows(ra), "y")
    rb = scatter_ring(rows(rb), "z")
    rc = scatter_ring(rows(rc), "x")
    flat = lambda r: [r[0][0], r[0][1], r[1][0], r[1][1]]
    fa = scatter_direct(flat(ra), "x")
    fb = scatter_direct(flat(rb), "y")
    fc = scatter_direct(flat(rc), "z")
    return jnp.concatenate([fa, fb, fc], axis=1).astype(BF)


def solution(mesh):
    in_specs = (P("ep", "etp"), P("ep", None), P("ep", None), P("ep", None, "etp"), P("ep", None, "etp"), P("ep", "etp", None))
    return jax.shard_map(body, mesh=mesh, in_specs=in_specs, out_specs=P("ep", "etp"), check_vma=False)
```

```python
import jax
import jax.numpy as jnp
from jax import lax
from jax.experimental import pallas as pl
from jax.experimental.pallas import tpu as pltpu
from jax.sharding import PartitionSpec as P


SIDE = 4
CAP = 24
TOK = 128
F = 512
K = SIDE * F
FF = 384
BF = jnp.bfloat16
F32 = jnp.float32
VMEM = 60 * 1024 * 1024
PIECES = [(s, dc) for dc in range(2) for s in range(SIDE)]


def ep_of(x, z, c):
    return ((x % SIDE) * SIDE + z % SIDE) * 2 + c


def recv(a, dim, d, flip=0):
    if dim == "y":
        return lax.ppermute(a, "etp", [((i + d) % SIDE, i) for i in range(SIDE)])
    dx, dz = (d, 0) if dim == "x" else (0, d)
    pairs = [(ep_of(x + dx, z + dz, c ^ flip), ep_of(x, z, c))
             for x in range(SIDE) for z in range(SIDE) for c in range(2)]
    return lax.ppermute(a, "ep", pairs)


def dot(a, b):
    return jnp.dot(a, b, preferred_element_type=F32)


def call(kernel, grid, in_specs, out_specs, out_shapes, scratch=()):
    return pl.pallas_call(
        kernel, grid=grid, in_specs=in_specs, out_specs=out_specs, out_shape=[jax.ShapeDtypeStruct(s, BF) for s in out_shapes],
        scratch_shapes=scratch,
        compiler_params=pltpu.CompilerParams(vmem_limit_bytes=VMEM, dimension_semantics=("arbitrary",) * len(grid)))


PAIRS = pl.BlockSpec((2, 256, 768), lambda i: (0, 0, 0))
NAMES = pl.BlockSpec((16, TOK), lambda i: (0, 0))
META = pl.BlockSpec((16, TOK), lambda i: (0, K // TOK))
DENSE = pl.BlockSpec((TOK, F), lambda i: (0, i))
ROWS = pl.BlockSpec((2, 96, F), lambda i: (0, 0, i))
ROWS_E = pl.BlockSpec((1, 96, K), lambda e: (e, 0, 0))


def select_body(names, *refs):
    xs, metas, outs, (p,) = refs[:4], refs[4:8], refs[8:16], refs[16:]

    @pl.when(pl.program_id(0) == 0)
    def _():
        shape = (TOK, TOK)
        before = jnp.where(lax.broadcasted_iota(jnp.int32, shape, 0) < lax.broadcasted_iota(jnp.int32, shape, 1), 1.0, 0.0).astype(BF)
        slot = lax.broadcasted_iota(jnp.int32, (CAP, TOK), 0).astype(F32)
        for g in range(4):
            ids = metas[g][...].astype(F32)
            match = jnp.zeros((16, TOK), F32)
            for k in range(8):
                match = match + jnp.where(ids[k:k + 1] == names[...], 1.0, 0.0)
            place = jnp.where(match > 0.0, dot(match.astype(BF), before), -1.0)
            for q in range(0, 16, 2):
                two = jnp.concatenate([jnp.where(place[q + e:q + e + 1] == slot, 1.0, 0.0) for e in range(2)], axis=0)
                p[g, q * CAP:q * CAP + 48, :] = two.astype(BF)

    for part in range(2):
        rows = [dot(p[g, part * 192:part * 192 + 192, :], xs[g][...]) for g in range(4)]
        for n in range(4):
            for e in range(2):
                at = n * 48 + e * CAP
                outs[part * 4 + n][e] = jnp.concatenate([r[at:at + CAP] for r in rows], axis=0).astype(BF)


def select(names, blocks):
    return call(select_body, (4,), [NAMES] + [DENSE] * 4 + [META] * 4, [ROWS] * 8, [(2, 96, K)] * 8,
                [pltpu.VMEM((4, 384, TOK), BF)])(names, *blocks, *blocks)


def combine_body(p, *refs):
    rows, outs = refs[:8], refs[8:]
    for k in range(2):
        picked = jnp.concatenate([r[e, k * 48:k * 48 + 48, :] for r in rows for e in range(2)], axis=0)
        dense = dot(p[k], picked).astype(BF)
        outs[2 * k][...] = dense[:TOK]
        outs[2 * k + 1][...] = dense[TOK:]


def combine(p, rows):
    return call(combine_body, (4,), [PAIRS] + [ROWS] * 8, [DENSE] * 4, [(TOK, K)] * 4)(p, *rows)


def weight_copies(y, e, wg, wu, wd, gu, dn, sems):
    copies = []
    for half in range(2):
        for dy in range(SIDE):
            n = (half * SIDE + dy) * 3
            src = pl.ds(pl.multiple_of(lax.rem(y + dy, SIDE) * 1024 + half * F, 128), F)
            dst = pl.ds(half * K + dy * F, F)
            copies.append(pltpu.make_async_copy(wg.at[e, src, :], gu.at[e, dst, pl.ds(0, FF)], sems.at[e, n]))
            copies.append(pltpu.make_async_copy(wu.at[e, src, :], gu.at[e, dst, pl.ds(FF, FF)], sems.at[e, n + 1]))
            copies.append(pltpu.make_async_copy(wd.at[e, :, src], dn.at[e, :, dst], sems.at[e, n + 2]))
    return copies


def experts_body(y_ref, *refs):
    a, b, (wg, wu, wd) = refs[:4], refs[4:8], refs[8:11]
    oa, ob, (gu, dn, first, acc, hs, sems) = refs[11:15], refs[15:19], refs[19:]
    e = pl.program_id(0)
    y = y_ref[0]

    @pl.when(e == 0)
    def _():
        for k in range(2):
            for cp in weight_copies(y, k, wg, wu, wd, gu, dn, sems):
                cp.start()

    for k in range(2):
        @pl.when(e == k)
        def _(k=k):
            for cp in weight_copies(y, k, wg, wu, wd, gu, dn, sems):
                cp.wait()

    first[...] = dot(jnp.concatenate([r[0] for r in a], axis=0), gu[e, 0:K, :])
    acc[...] = dot(jnp.concatenate([r[0] for r in b], axis=0), gu[e, K:2 * K, :])
    for i in range(SIDE):
        for j in range(SIDE):
            to, fro = (i * SIDE + j) * CAP, (j * SIDE + i) * CAP
            v = acc[to:to + CAP, :] + first[fro:fro + CAP, :]
            g, u = v[:, :FF], v[:, FF:]
            hs[to:to + CAP, :] = g * (1.0 / (1.0 + jnp.exp(-g))) * u
    h2 = hs[...].astype(BF)
    h1 = jnp.concatenate([hs[(j * SIDE + i) * CAP:(j * SIDE + i + 1) * CAP, :] for i in range(SIDE) for j in range(SIDE)], axis=0).astype(BF)
    ra = dot(h1, dn[e, :, 0:K]).astype(BF)
    rb = dot(h2, dn[e, :, K:2 * K]).astype(BF)
    for s in range(SIDE):
        oa[s][0] = ra[s * 96:(s + 1) * 96]
        ob[s][0] = rb[s * 96:(s + 1) * 96]


def experts(y, a, b, wg, wu, wd):
    hbm = pl.BlockSpec(memory_space=pl.ANY)
    scratch = [pltpu.VMEM((2, 2 * K, 2 * FF), BF), pltpu.VMEM((2, FF, 2 * K), BF), pltpu.VMEM((384, 2 * FF), F32),
               pltpu.VMEM((384, 2 * FF), F32), pltpu.VMEM((384, FF), F32), pltpu.SemaphoreType.DMA((2, 24))]
    o = call(experts_body, (2,), [pl.BlockSpec(memory_space=pltpu.SMEM)] + [ROWS_E] * 8 + [hbm] * 3, [ROWS_E] * 8,
             [(2, 96, K)] * 8, scratch)(y, *a, *b, wg, wu, wd)
    return o[:4], o[4:]


def weighted_table(info, names):
    columns = jnp.stack(info).astype(F32)
    ids, prob = columns[:, :8], columns[:, 8:]
    hit = ids[:, None, :, :] == names[None, :, None, None]
    match = jnp.any(hit, axis=2)
    weight = jnp.sum(jnp.where(hit, prob[:, None, :, :], 0.0), axis=2)
    t = jnp.arange(TOK)
    before = (t[:, None] < t[None, :]).astype(BF)
    place = jnp.einsum("get,tu->geu", match.astype(BF), before, preferred_element_type=F32)
    place = jnp.where(match, place, -1.0).reshape(2, 2, 16, TOK).transpose(0, 2, 1, 3)
    weight = weight.reshape(2, 2, 16, TOK).transpose(0, 2, 1, 3)
    eye = jnp.arange(2)
    same = (eye[:, None] == eye[None, :])[None, None, :, None, :, None]
    on = (place[:, :, None, None, :, :] == jnp.arange(CAP, dtype=F32)[None, None, None, :, None, None]) & same
    wgt = jnp.where(on, weight[:, :, None, None, :, :], 0.0).astype(BF)
    return wgt.reshape(2, 768, 256).swapaxes(1, 2)


def total(terms):
    out = terms[0].astype(F32)
    for t in terms[1:]:
        out = out + t.astype(F32)
    return out


def body(tokens, expert_ids, gate_prob, gate_weight, up_weight, down_weight):
    ep = lax.axis_index("ep")
    x, z, c = ep // 8, (ep // 2) % SIDE, ep % 2
    y = lax.axis_index("etp").astype(jnp.int32).reshape(1)
    meta = jnp.concatenate([expert_ids.T.astype(BF), gate_prob.T.astype(BF), jnp.zeros((112, TOK), BF)], axis=0)
    wide = [tokens] + [recv(tokens, "y", d) for d in (1, 2, 3)]
    msg = [jnp.concatenate([w[:, h * F:(h + 1) * F] for w in wide] + [meta], axis=1) for h in range(2)]
    axes = (("x", "z"), ("z", "x"))
    near, rows, names, got = [None] * 2, [None] * 2, [None] * 2, [None] * 2
    for h, (dim, far) in enumerate(axes):
        near[h] = [msg[h]] + [recv(msg[h], dim, d) for d in (1, 2, 3)]
        mates = []
        for s, dc in PIECES:
            mate = ep_of(x, z + s, c ^ dc) if far == "z" else ep_of(x + s, z, c ^ dc)
            mates += [2 * mate, 2 * mate + 1]
        names[h] = jnp.stack(mates).astype(F32)
        picked = select(jnp.broadcast_to(names[h][:, None], (16, TOK)), near[h])
        rows[h] = {}
        for s, dc in PIECES:
            out = picked[PIECES.index(((-s) % SIDE, dc))]
            rows[h][s, dc] = out if (s, dc) == (0, 0) else recv(out, far, s, dc)
        got[h] = {}
    for dc in range(2):
        outs = experts(y, *[[rows[h][s, dc] for s in range(SIDE)] for h in range(2)], gate_weight, up_weight, down_weight)
        for h, (dim, far) in enumerate(axes):
            for s in range(SIDE):
                out = outs[h][(-s) % SIDE]
                got[h][s, dc] = out if (s, dc) == (0, 0) else recv(out, far, s, dc)
    halves = []
    for h, (dim, far) in enumerate(axes):
        weighted = weighted_table([m[:16, K:] for m in near[h]], names[h])
        dense = combine(weighted, [got[h][q] for q in PIECES])
        halves.append(total([dense[0]] + [recv(dense[d], dim, -d) for d in (1, 2, 3)]).astype(BF))
    parts = [jnp.concatenate([halves[h][:, d * F:(d + 1) * F] for h in range(2)], axis=1) for d in range(SIDE)]
    return total([parts[0]] + [recv(parts[d], "y", -d) for d in (1, 2, 3)]).astype(BF)


def solution(mesh):
    in_specs = (P("ep", "etp"), P("ep", None), P("ep", None), P("ep", None, "etp"), P("ep", None, "etp"), P("ep", "etp", None))

    return jax.shard_map(body, mesh=mesh, in_specs=in_specs, out_specs=P("ep", "etp"), check_vma=False)
```

```python
import jax
import jax.numpy as jnp
from jax import lax
from jax.experimental import pallas as pl
from jax.experimental.pallas import tpu as pltpu
from jax.sharding import PartitionSpec as P


SIDE = 4
CAP = 24
TOK = 128
F = 512
K = SIDE * F
FF = 384
BF = jnp.bfloat16
F32 = jnp.float32
VMEM = 60 * 1024 * 1024
PIECES = [(s, dc) for dc in range(2) for s in range(SIDE)]


def ep_of(x, z, c):
    return ((x % SIDE) * SIDE + z % SIDE) * 2 + c


def recv(a, dim, d, flip=0):
    if dim == "y":
        return lax.ppermute(a, "etp", [((i + d) % SIDE, i) for i in range(SIDE)])
    dx, dz = (d, 0) if dim == "x" else (0, d)
    pairs = [(ep_of(x + dx, z + dz, c ^ flip), ep_of(x, z, c))
             for x in range(SIDE) for z in range(SIDE) for c in range(2)]
    return lax.ppermute(a, "ep", pairs)


def dot(a, b):
    return jnp.dot(a, b, preferred_element_type=F32)


def call(kernel, grid, in_specs, out_specs, out_shapes, scratch=()):
    return pl.pallas_call(
        kernel, grid=grid, in_specs=in_specs, out_specs=out_specs, out_shape=[jax.ShapeDtypeStruct(s, BF) for s in out_shapes],
        scratch_shapes=scratch,
        compiler_params=pltpu.CompilerParams(vmem_limit_bytes=VMEM, dimension_semantics=("arbitrary",) * len(grid)))


PAIRS = pl.BlockSpec((2, 256, 768), lambda i: (0, 0, 0))
COLS = 512
META = pl.BlockSpec((16, TOK), lambda i: (0, K // TOK))
DENSE = pl.BlockSpec((TOK, COLS), lambda i: (0, i))
PART = pl.BlockSpec((TOK // 2, COLS), lambda i: (0, i))
ROWS = pl.BlockSpec((2, 96, COLS), lambda i: (0, 0, i))
NEAR = [DENSE, DENSE, PART, PART, DENSE]


def select_body(where, *refs):
    xs, metas, outs, (p,) = refs[:10], refs[10:18], refs[18:34], refs[34:]

    @pl.when(pl.program_id(0) == 0)
    def _():
        shape = (TOK, TOK)
        before = jnp.where(lax.broadcasted_iota(jnp.int32, shape, 0) < lax.broadcasted_iota(jnp.int32, shape, 1), 1.0, 0.0).astype(BF)
        slot = lax.broadcasted_iota(jnp.int32, (CAP, TOK), 0).astype(F32)
        q = lax.broadcasted_iota(jnp.int32, (16, TOK), 0)
        step, flip = (q // 2) % SIDE, q // 8
        x, z, c = where[0], where[1], where[2]
        core = jnp.where(flip == 1, 1 - c, c)
        for h in range(2):
            zz = (z + step) % SIDE if h == 0 else z
            xx = x if h == 0 else (x + step) % SIDE
            names = (((xx * SIDE + zz) * 2 + core) * 2 + q % 2).astype(F32)
            for g in range(4):
                ids = metas[h * 4 + g][...].astype(F32)
                match = jnp.zeros((16, TOK), F32)
                for k in range(8):
                    match = match + jnp.where(ids[k:k + 1] == names, 1.0, 0.0)
                place = jnp.where(match > 0.0, dot(match.astype(BF), before), -1.0)
                for n in range(0, 16, 2):
                    two = jnp.concatenate([jnp.where(place[n + e:n + e + 1] == slot, 1.0, 0.0) for e in range(2)], axis=0)
                    p[h * 4 + g, n * CAP:n * CAP + 48, :] = two.astype(BF)

    for h in range(2):
        x0, x1, x2a, x2b, x3 = [r[...] for r in xs[h * 5:h * 5 + 5]]
        dense = [x0, x1, jnp.concatenate([x2a, x2b], axis=0), x3]
        for part in range(2):
            rows = [dot(p[h * 4 + g, part * 192:part * 192 + 192, :], dense[g]) for g in range(4)]
            for n in range(4):
                for e in range(2):
                    at = n * 48 + e * CAP
                    outs[h * 8 + part * 4 + n][e] = jnp.concatenate([r[at:at + CAP] for r in rows], axis=0).astype(BF)


def select(where, near):
    metas = [b for n in near for b in (n[0], n[1], n[2], n[4])]
    return call(select_body, (K // COLS,), [pl.BlockSpec(memory_space=pltpu.SMEM)] + NEAR * 2 + [META] * 8, [ROWS] * 16, [(2, 96, K)] * 16,
                [pltpu.VMEM((8, 384, TOK), BF)])(where, *near[0], *near[1], *metas)


def combine_body(*refs):
    tables, rows, outs = refs[:2], refs[2:18], refs[18:]
    for h in range(2):
        o = outs[h * 7:h * 7 + 7]
        for k in range(2):
            picked = jnp.concatenate([r[e, k * 48:k * 48 + 48, :] for r in rows[h * 8:h * 8 + 8] for e in range(2)], axis=0)
            dense = dot(tables[h][k], picked).astype(BF)
            quarters = [dense[n * 64:n * 64 + 64] for n in range(4)]
            if k == 0:
                o[0][...] = dense[:TOK]
                quarters = quarters[2:]
            for n, part in enumerate(quarters):
                o[(1 if k == 0 else 3) + n][...] = part


def combine(tables, rows):
    shapes = [(TOK, K)] + [(TOK // 2, K)] * 6
    return call(combine_body, (K // COLS,), [PAIRS] * 2 + [ROWS] * 16, ([DENSE] + [PART] * 6) * 2, shapes * 2)(*tables, *rows[0], *rows[1])


def experts_body(y_ref, *refs):
    pieces, (wg, wu, wd), outs = refs[:8], refs[8:11], refs[11:19]
    gate, up, down, lhs, acc, hs, hid, res, sems, out_sems = refs[19:]
    e = pl.program_id(0)
    y = y_ref[0]

    def stage(k, n):
        if n == 2:
            return [pltpu.make_async_copy(wd.at[k], down.at[k], sems.at[k, 24])]
        copies = []
        for s in range(SIDE):
            copies.append(pltpu.make_async_copy(pieces[n * SIDE + s].at[k], lhs.at[k, n, pl.ds(s * 96, 96), :], sems.at[k, n * 12 + s]))
        for dy in range(SIDE):
            src = pl.ds(pl.multiple_of(lax.rem(y + dy, SIDE) * 1024 + n * F, 128), F)
            dst = pl.ds(n * K + dy * F, F)
            copies.append(pltpu.make_async_copy(wg.at[k, src, :], gate.at[k, dst, :], sems.at[k, n * 12 + 4 + dy]))
            copies.append(pltpu.make_async_copy(wu.at[k, src, :], up.at[k, dst, :], sems.at[k, n * 12 + 8 + dy]))
        return copies

    def start(k, n):
        for cp in stage(k, n):
            cp.start()

    def wait(n):
        for cp in stage(e, n):
            cp.wait()

    def results(k, half):
        return [pltpu.make_async_copy(res.at[k, half, pl.ds(s * 96, 96), :], outs[half * SIDE + s].at[k], out_sems.at[k, half * SIDE + s])
                for s in range(SIDE)]

    @pl.when(e == 0)
    def _():
        for k in range(2):
            for n in range(3):
                start(k, n)

    @pl.loop(0, 2)
    def _(half):
        for n in range(2):
            @pl.when(half == n)
            def _(n=n):
                wait(n)
        rows = pl.ds(pl.multiple_of(half * K, K), K)
        for n, w in enumerate((gate, up)):
            acc[half, :, n * FF:(n + 1) * FF] = dot(lhs[e, half], w[e, rows, :])

    @pl.loop(0, SIDE * SIDE)
    def _(n):
        to = pl.ds(pl.multiple_of(n * CAP, 8), CAP)
        fro = pl.ds(pl.multiple_of(((n % SIDE) * SIDE + n // SIDE) * CAP, 8), CAP)
        v = acc[1, to, :] + acc[0, fro, :]
        g, u = v[:, :FF], v[:, FF:]
        hs[to, :] = g * (1.0 / (1.0 + jnp.exp(-g))) * u

    hid[0] = jnp.concatenate([hs[(j * SIDE + i) * CAP:(j * SIDE + i + 1) * CAP, :] for i in range(SIDE) for j in range(SIDE)], axis=0).astype(BF)
    hid[1] = hs[...].astype(BF)
    wait(2)

    @pl.loop(0, 2 * SIDE)
    def _(n):
        half, dy = n // SIDE, n % SIDE
        src = pl.ds(pl.multiple_of(lax.rem(y + dy, SIDE) * 1024 + half * F, F), F)
        res[e, half, :, pl.ds(pl.multiple_of(dy * F, F), F)] = dot(hid[half], down[e, :, src]).astype(BF)
        for k in range(2):
            @pl.when(n == k * SIDE + SIDE - 1)
            def _(k=k):
                for cp in results(e, k):
                    cp.start()

    @pl.when(e == 1)
    def _():
        for k in range(2):
            for half in range(2):
                for cp in results(k, half):
                    cp.wait()


def experts(y, a, b, wg, wu, wd):
    hbm = pl.BlockSpec(memory_space=pl.ANY)
    scratch = [pltpu.VMEM((2, 2 * K, FF), BF), pltpu.VMEM((2, 2 * K, FF), BF), pltpu.VMEM((2, FF, 2 * K), BF), pltpu.VMEM((2, 2, 384, K), BF),
               pltpu.VMEM((2, 384, 2 * FF), F32), pltpu.VMEM((384, FF), F32), pltpu.VMEM((2, 384, FF), BF), pltpu.VMEM((2, 2, 384, K), BF),
               pltpu.SemaphoreType.DMA((2, 25)), pltpu.SemaphoreType.DMA((2, 8))]
    o = call(experts_body, (2,), [pl.BlockSpec(memory_space=pltpu.SMEM)] + [hbm] * 11, [hbm] * 8,
             [(2, 96, K)] * 8, scratch)(y, *a, *b, wg, wu, wd)
    return o[:4], o[4:]


def weighted_table(info, names):
    columns = jnp.stack(info).astype(F32)
    ids, prob = columns[:, :8], columns[:, 8:]
    hit = ids[:, None, :, :] == names[None, :, None, None]
    match = jnp.any(hit, axis=2)
    weight = jnp.sum(jnp.where(hit, prob[:, None, :, :], 0.0), axis=2)
    t = jnp.arange(TOK)
    before = (t[:, None] < t[None, :]).astype(BF)
    place = jnp.einsum("get,tu->geu", match.astype(BF), before, preferred_element_type=F32)
    place = jnp.where(match, place, -1.0).reshape(2, 2, 16, TOK).transpose(0, 2, 1, 3)
    weight = weight.reshape(2, 2, 16, TOK).transpose(0, 2, 1, 3)
    eye = jnp.arange(2)
    same = (eye[:, None] == eye[None, :])[None, None, :, None, :, None]
    on = (place[:, :, None, None, :, :] == jnp.arange(CAP, dtype=F32)[None, None, None, :, None, None]) & same
    wgt = jnp.where(on, weight[:, :, None, None, :, :], 0.0).astype(BF)
    return wgt.reshape(2, 768, 256).swapaxes(1, 2)


def total(terms):
    out = terms[0].astype(F32)
    for t in terms[1:]:
        out = out + t.astype(F32)
    return out


def gather_ring(a, dim):
    half = a.shape[0] // 2
    r1, r3 = recv(a, dim, 1), recv(a, dim, -1)
    return [a, r1, recv(r1[:half], dim, 1), recv(r3[half:], dim, -1), r3]


def scatter_ring(blocks, dim):
    b0, b10, b11, b20, b21, b30, b31 = blocks
    s0, s1 = recv(b20, dim, -1), recv(b21, dim, 1)
    i1, j0 = recv(b11, dim, -1), recv(b30, dim, 1)
    i0 = recv(total([b10, s0]).astype(BF), dim, -1)
    j1 = recv(total([b31, s1]).astype(BF), dim, 1)
    half = b20.shape[0]
    return jnp.concatenate([total([b0[:half], i0, j0]), total([b0[half:], i1, j1])], axis=0)


def body(tokens, expert_ids, gate_prob, gate_weight, up_weight, down_weight):
    ep = lax.axis_index("ep")
    x, z, c = ep // 8, (ep // 2) % SIDE, ep % 2
    where = jnp.stack([x, z, c]).astype(jnp.int32)
    y = lax.axis_index("etp").astype(jnp.int32).reshape(1)
    meta = jnp.concatenate([expert_ids.T.astype(BF), gate_prob.T.astype(BF), jnp.zeros((112, TOK), BF)], axis=0)
    wide = [tokens] + [recv(tokens, "y", d) for d in (1, 2, 3)]
    axes = (("x", "z"), ("z", "x"))
    near = [gather_ring(jnp.concatenate([w[:, h * F:(h + 1) * F] for w in wide] + [meta], axis=1), dim)
            for h, (dim, far) in enumerate(axes)]
    picked = select(where, near)
    rows, got, tables = [{}, {}], [{}, {}], []
    for h, (dim, far) in enumerate(axes):
        mates = []
        for s, dc in PIECES:
            mate = ep_of(x, z + s, c ^ dc) if far == "z" else ep_of(x + s, z, c ^ dc)
            mates += [2 * mate, 2 * mate + 1]
            out = picked[h * 8 + PIECES.index(((-s) % SIDE, dc))]
            rows[h][s, dc] = out if (s, dc) == (0, 0) else recv(out, far, s, dc)
        n = near[h]
        tables.append(weighted_table([m[:16, K:] for m in (n[0], n[1], n[2], n[4])], jnp.stack(mates).astype(F32)))
    for dc in range(2):
        outs = experts(y, *[[rows[h][s, dc] for s in range(SIDE)] for h in range(2)], gate_weight, up_weight, down_weight)
        for h, (dim, far) in enumerate(axes):
            for s in range(SIDE):
                out = outs[h][(-s) % SIDE]
                got[h][s, dc] = out if (s, dc) == (0, 0) else recv(out, far, s, dc)
    dense = combine(tables, [[got[h][q] for q in PIECES] for h in range(2)])
    halves = [scatter_ring(dense[h * 7:h * 7 + 7], dim).astype(BF) for h, (dim, far) in enumerate(axes)]
    parts = [jnp.concatenate([halves[h][:, d * F:(d + 1) * F] for h in range(2)], axis=1) for d in range(SIDE)]
    return total([parts[0]] + [recv(parts[d], "y", -d) for d in (1, 2, 3)]).astype(BF)


def solution(mesh):
    in_specs = (P("ep", "etp"), P("ep", None), P("ep", None), P("ep", None, "etp"), P("ep", None, "etp"), P("ep", "etp", None))

    return jax.shard_map(body, mesh=mesh, in_specs=in_specs, out_specs=P("ep", "etp"), check_vma=False)
```

```python
import jax
import jax.numpy as jnp
from jax import lax
from jax.experimental import pallas as pl
from jax.experimental.pallas import tpu as pltpu
from jax.sharding import PartitionSpec as P


SIDE = 4
CAP = 24
TOK = 128
F = 512
K = SIDE * F
FF = 384
BF = jnp.bfloat16
F32 = jnp.float32
VMEM = 60 * 1024 * 1024
PIECES = [(s, dc) for dc in range(2) for s in range(SIDE)]


def ep_of(x, z, c):
    return ((x % SIDE) * SIDE + z % SIDE) * 2 + c


def recv(a, dim, d, flip=0):
    if dim == "y":
        return lax.ppermute(a, "etp", [((i + d) % SIDE, i) for i in range(SIDE)])
    dx, dz = (d, 0) if dim == "x" else (0, d)
    pairs = [(ep_of(x + dx, z + dz, c ^ flip), ep_of(x, z, c))
             for x in range(SIDE) for z in range(SIDE) for c in range(2)]
    return lax.ppermute(a, "ep", pairs)


def dot(a, b):
    return jnp.dot(a, b, preferred_element_type=F32)


def call(kernel, grid, in_specs, out_specs, out_shapes, scratch=()):
    return pl.pallas_call(
        kernel, grid=grid, in_specs=in_specs, out_specs=out_specs, out_shape=[jax.ShapeDtypeStruct(s, BF) for s in out_shapes],
        scratch_shapes=scratch,
        compiler_params=pltpu.CompilerParams(vmem_limit_bytes=VMEM, dimension_semantics=("arbitrary",) * len(grid)))


PAIRS = pl.BlockSpec((2, 256, 768), lambda i: (0, 0, 0))
COLS = 1024
META = pl.BlockSpec((16, TOK), lambda i: (0, K // TOK))
DENSE = pl.BlockSpec((TOK, COLS), lambda i: (0, i))
PART = pl.BlockSpec((TOK // 2, COLS), lambda i: (0, i))
ROWS = pl.BlockSpec((2, 96, COLS), lambda i: (0, 0, i))
NEAR = [DENSE, DENSE, PART, PART, DENSE]


def select_body(where, *refs):
    xs, metas, outs, (p,) = refs[:10], refs[10:18], refs[18:34], refs[34:]

    @pl.when(pl.program_id(0) == 0)
    def _():
        shape = (TOK, TOK)
        before = jnp.where(lax.broadcasted_iota(jnp.int32, shape, 0) < lax.broadcasted_iota(jnp.int32, shape, 1), 1.0, 0.0).astype(BF)
        slot = lax.broadcasted_iota(jnp.int32, (CAP, TOK), 0).astype(F32)
        q = lax.broadcasted_iota(jnp.int32, (16, TOK), 0)
        step, flip = (q // 2) % SIDE, q // 8
        x, z, c = where[0], where[1], where[2]
        core = jnp.where(flip == 1, 1 - c, c)
        for h in range(2):
            zz = (z + step) % SIDE if h == 0 else z
            xx = x if h == 0 else (x + step) % SIDE
            names = (((xx * SIDE + zz) * 2 + core) * 2 + q % 2).astype(F32)
            for g in range(4):
                ids = metas[h * 4 + g][...].astype(F32)
                match = jnp.zeros((16, TOK), F32)
                for k in range(8):
                    match = match + jnp.where(ids[k:k + 1] == names, 1.0, 0.0)
                place = jnp.where(match > 0.0, dot(match.astype(BF), before), -1.0)
                for n in range(0, 16, 2):
                    two = jnp.concatenate([jnp.where(place[n + e:n + e + 1] == slot, 1.0, 0.0) for e in range(2)], axis=0)
                    p[h * 4 + g, n * CAP:n * CAP + 48, :] = two.astype(BF)

    for h in range(2):
        x0, x1, x2a, x2b, x3 = [r[...] for r in xs[h * 5:h * 5 + 5]]
        dense = [x0, x1, jnp.concatenate([x2a, x2b], axis=0), x3]
        for part in range(2):
            rows = [dot(p[h * 4 + g, part * 192:part * 192 + 192, :], dense[g]) for g in range(4)]
            for n in range(4):
                for e in range(2):
                    at = n * 48 + e * CAP
                    outs[h * 8 + part * 4 + n][e] = jnp.concatenate([r[at:at + CAP] for r in rows], axis=0).astype(BF)


def select(where, near):
    metas = [b for n in near for b in (n[0], n[1], n[2], n[4])]
    return call(select_body, (K // COLS,), [pl.BlockSpec(memory_space=pltpu.SMEM)] + NEAR * 2 + [META] * 8, [ROWS] * 16, [(2, 96, K)] * 16,
                [pltpu.VMEM((8, 384, TOK), BF)])(where, *near[0], *near[1], *metas)


def combine_body(*refs):
    tables, rows, outs = refs[:2], refs[2:18], refs[18:]
    for h in range(2):
        o = outs[h * 7:h * 7 + 7]
        for k in range(2):
            picked = jnp.concatenate([r[e, k * 48:k * 48 + 48, :] for r in rows[h * 8:h * 8 + 8] for e in range(2)], axis=0)
            dense = dot(tables[h][k], picked).astype(BF)
            quarters = [dense[n * 64:n * 64 + 64] for n in range(4)]
            if k == 0:
                o[0][...] = dense[:TOK]
                quarters = quarters[2:]
            for n, part in enumerate(quarters):
                o[(1 if k == 0 else 3) + n][...] = part


def combine(tables, rows):
    shapes = [(TOK, K)] + [(TOK // 2, K)] * 6
    return call(combine_body, (K // COLS,), [PAIRS] * 2 + [ROWS] * 16, ([DENSE] + [PART] * 6) * 2, shapes * 2)(*tables, *rows[0], *rows[1])


def experts_body(y_ref, *refs):
    pieces, (wg, wu, wd), outs = refs[:8], refs[8:11], refs[11:19]
    gu, down, lhs, acc, hs, hid, res, sems, out_sems = refs[19:]
    e = pl.program_id(0)
    y = y_ref[0]

    def stage(k, n):
        if n == 2:
            return [pltpu.make_async_copy(wd.at[k], down.at[k], sems.at[k, 24])]
        copies = []
        for s in range(SIDE):
            copies.append(pltpu.make_async_copy(pieces[n * SIDE + s].at[k], lhs.at[k, n, pl.ds(s * 96, 96), :], sems.at[k, n * 12 + s]))
        for dy in range(SIDE):
            src = pl.ds(pl.multiple_of(lax.rem(y + dy, SIDE) * 1024 + n * F, 128), F)
            dst = pl.ds(n * K + dy * F, F)
            copies.append(pltpu.make_async_copy(wg.at[k, src, :], gu.at[0, k, dst, :], sems.at[k, n * 12 + 4 + dy]))
            copies.append(pltpu.make_async_copy(wu.at[k, src, :], gu.at[1, k, dst, :], sems.at[k, n * 12 + 8 + dy]))
        return copies

    def start(k, n):
        for cp in stage(k, n):
            cp.start()

    def wait(n):
        for cp in stage(e, n):
            cp.wait()

    def results(k, half):
        return [pltpu.make_async_copy(res.at[k, half, pl.ds(s * 96, 96), :], outs[half * SIDE + s].at[k], out_sems.at[k, half * SIDE + s])
                for s in range(SIDE)]

    @pl.when(e == 0)
    def _():
        for k in range(2):
            for n in range(3):
                start(k, n)

    @pl.loop(0, 4)
    def _(n):
        half, kind = n // 2, n % 2
        for k in range(2):
            @pl.when(n == 2 * k)
            def _(k=k):
                wait(k)
        acc[kind, half] = dot(lhs[e, half], gu[kind, e, pl.ds(pl.multiple_of(half * K, K), K), :])

    @pl.loop(0, SIDE * SIDE)
    def _(n):
        to = pl.ds(pl.multiple_of(n * CAP, 8), CAP)
        fro = pl.ds(pl.multiple_of(((n % SIDE) * SIDE + n // SIDE) * CAP, 8), CAP)
        g = acc[0, 1, to, :] + acc[0, 0, fro, :]
        u = acc[1, 1, to, :] + acc[1, 0, fro, :]
        hs[to, :] = g * (1.0 / (1.0 + jnp.exp(-g))) * u

    hid[0] = jnp.concatenate([hs[(j * SIDE + i) * CAP:(j * SIDE + i + 1) * CAP, :] for i in range(SIDE) for j in range(SIDE)], axis=0).astype(BF)
    hid[1] = hs[...].astype(BF)
    wait(2)

    @pl.loop(0, 2 * SIDE)
    def _(n):
        half, dy = n // SIDE, n % SIDE
        src = pl.ds(pl.multiple_of(lax.rem(y + dy, SIDE) * 1024 + half * F, F), F)
        res[e, half, :, pl.ds(pl.multiple_of(dy * F, F), F)] = dot(hid[half], down[e, :, src]).astype(BF)
        for k in range(2):
            @pl.when(n == k * SIDE + SIDE - 1)
            def _(k=k):
                for cp in results(e, k):
                    cp.start()

    @pl.when(e == 1)
    def _():
        for k in range(2):
            for half in range(2):
                for cp in results(k, half):
                    cp.wait()


def experts(y, a, b, wg, wu, wd):
    hbm = pl.BlockSpec(memory_space=pl.ANY)
    scratch = [pltpu.VMEM((2, 2, 2 * K, FF), BF), pltpu.VMEM((2, FF, 2 * K), BF), pltpu.VMEM((2, 2, 384, K), BF),
               pltpu.VMEM((2, 2, 384, FF), F32), pltpu.VMEM((384, FF), F32), pltpu.VMEM((2, 384, FF), BF), pltpu.VMEM((2, 2, 384, K), BF),
               pltpu.SemaphoreType.DMA((2, 25)), pltpu.SemaphoreType.DMA((2, 8))]
    o = call(experts_body, (2,), [pl.BlockSpec(memory_space=pltpu.SMEM)] + [hbm] * 11, [hbm] * 8,
             [(2, 96, K)] * 8, scratch)(y, *a, *b, wg, wu, wd)
    return o[:4], o[4:]


def weighted_table(info, names):
    columns = jnp.stack(info).astype(F32)
    ids, prob = columns[:, :8], columns[:, 8:]
    hit = ids[:, None, :, :] == names[None, :, None, None]
    match = jnp.any(hit, axis=2)
    weight = jnp.sum(jnp.where(hit, prob[:, None, :, :], 0.0), axis=2)
    t = jnp.arange(TOK)
    before = (t[:, None] < t[None, :]).astype(BF)
    place = jnp.einsum("get,tu->geu", match.astype(BF), before, preferred_element_type=F32)
    place = jnp.where(match, place, -1.0).reshape(2, 2, 16, TOK).transpose(0, 2, 1, 3)
    weight = weight.reshape(2, 2, 16, TOK).transpose(0, 2, 1, 3)
    eye = jnp.arange(2)
    same = (eye[:, None] == eye[None, :])[None, None, :, None, :, None]
    on = (place[:, :, None, None, :, :] == jnp.arange(CAP, dtype=F32)[None, None, None, :, None, None]) & same
    wgt = jnp.where(on, weight[:, :, None, None, :, :], 0.0).astype(BF)
    return wgt.reshape(2, 768, 256).swapaxes(1, 2)


def total(terms):
    out = terms[0].astype(F32)
    for t in terms[1:]:
        out = out + t.astype(F32)
    return out


def gather_ring(a, dim):
    half = a.shape[0] // 2
    r1, r3 = recv(a, dim, 1), recv(a, dim, -1)
    return [a, r1, recv(r1[:half], dim, 1), recv(r3[half:], dim, -1), r3]


def scatter_ring(blocks, dim):
    b0, b10, b11, b20, b21, b30, b31 = blocks
    s0, s1 = recv(b20, dim, -1), recv(b21, dim, 1)
    i1, j0 = recv(b11, dim, -1), recv(b30, dim, 1)
    i0 = recv(total([b10, s0]).astype(BF), dim, -1)
    j1 = recv(total([b31, s1]).astype(BF), dim, 1)
    half = b20.shape[0]
    return jnp.concatenate([total([b0[:half], i0, j0]), total([b0[half:], i1, j1])], axis=0)


def body(tokens, expert_ids, gate_prob, gate_weight, up_weight, down_weight):
    ep = lax.axis_index("ep")
    x, z, c = ep // 8, (ep // 2) % SIDE, ep % 2
    where = jnp.stack([x, z, c]).astype(jnp.int32)
    y = lax.axis_index("etp").astype(jnp.int32).reshape(1)
    meta = jnp.concatenate([expert_ids.T.astype(BF), gate_prob.T.astype(BF), jnp.zeros((112, TOK), BF)], axis=0)
    wide = [tokens] + [recv(tokens, "y", d) for d in (1, 2, 3)]
    axes = (("x", "z"), ("z", "x"))
    near = [gather_ring(jnp.concatenate([w[:, h * F:(h + 1) * F] for w in wide] + [meta], axis=1), dim)
            for h, (dim, far) in enumerate(axes)]
    picked = select(where, near)
    rows, got, tables = [{}, {}], [{}, {}], []
    for h, (dim, far) in enumerate(axes):
        mates = []
        for s, dc in PIECES:
            mate = ep_of(x, z + s, c ^ dc) if far == "z" else ep_of(x + s, z, c ^ dc)
            mates += [2 * mate, 2 * mate + 1]
            out = picked[h * 8 + PIECES.index(((-s) % SIDE, dc))]
            rows[h][s, dc] = out if (s, dc) == (0, 0) else recv(out, far, s, dc)
        n = near[h]
        tables.append(weighted_table([m[:16, K:] for m in (n[0], n[1], n[2], n[4])], jnp.stack(mates).astype(F32)))
    for dc in range(2):
        outs = experts(y, *[[rows[h][s, dc] for s in range(SIDE)] for h in range(2)], gate_weight, up_weight, down_weight)
        for h, (dim, far) in enumerate(axes):
            for s in range(SIDE):
                out = outs[h][(-s) % SIDE]
                got[h][s, dc] = out if (s, dc) == (0, 0) else recv(out, far, s, dc)
    dense = combine(tables, [[got[h][q] for q in PIECES] for h in range(2)])
    halves = [scatter_ring(dense[h * 7:h * 7 + 7], dim).astype(BF) for h, (dim, far) in enumerate(axes)]
    parts = [jnp.concatenate([halves[h][:, d * F:(d + 1) * F] for h in range(2)], axis=1) for d in range(SIDE)]
    return total([parts[0]] + [recv(parts[d], "y", -d) for d in (1, 2, 3)]).astype(BF)


def solution(mesh):
    in_specs = (P("ep", "etp"), P("ep", None), P("ep", None), P("ep", None, "etp"), P("ep", None, "etp"), P("ep", "etp", None))

    return jax.shard_map(body, mesh=mesh, in_specs=in_specs, out_specs=P("ep", "etp"), check_vma=False)
```

```python
import jax
import jax.numpy as jnp
from jax import lax
from jax.experimental import pallas as pl
from jax.experimental.pallas import tpu as pltpu
from jax.sharding import PartitionSpec as P


SIDE = 4
CAP = 24
TOK = 128
F = 512
K = SIDE * F
FF = 384
BF = jnp.bfloat16
F32 = jnp.float32
MIB = 1024 * 1024
PIECES = [(s, dc) for dc in range(2) for s in range(SIDE)]


def ep_of(x, z, c):
    return ((x % SIDE) * SIDE + z % SIDE) * 2 + c


def recv(a, dim, d, flip=0):
    if dim == "y":
        return lax.ppermute(a, "etp", [((i + d) % SIDE, i) for i in range(SIDE)])
    dx, dz = (d, 0) if dim == "x" else (0, d)
    pairs = [(ep_of(x + dx, z + dz, c ^ flip), ep_of(x, z, c))
             for x in range(SIDE) for z in range(SIDE) for c in range(2)]
    return lax.ppermute(a, "ep", pairs)


def dot(a, b):
    return jnp.dot(a, b, preferred_element_type=F32)


def call(kernel, grid, in_specs, out_specs, out_shapes, scratch=(), mib=28):
    return pl.pallas_call(
        kernel, grid=grid, in_specs=in_specs, out_specs=out_specs, out_shape=[jax.ShapeDtypeStruct(s, BF) for s in out_shapes],
        scratch_shapes=scratch,
        compiler_params=pltpu.CompilerParams(vmem_limit_bytes=mib * MIB, dimension_semantics=("arbitrary",) * len(grid)))


PAIRS = pl.BlockSpec((2, 256, 768), lambda i: (0, 0, 0))
COLS = 1024
META = pl.BlockSpec((16, TOK), lambda i: (0, K // TOK))
DENSE = pl.BlockSpec((TOK, COLS), lambda i: (0, i))
PART = pl.BlockSpec((TOK // 2, COLS), lambda i: (0, i))
ROWS = pl.BlockSpec((2, 96, COLS), lambda i: (0, 0, i))
NEAR = [DENSE, DENSE, PART, PART, DENSE]


def select_body(where, *refs):
    xs, metas, outs, (p,) = refs[:10], refs[10:18], refs[18:34], refs[34:]

    @pl.when(pl.program_id(0) == 0)
    def _():
        shape = (TOK, TOK)
        before = jnp.where(lax.broadcasted_iota(jnp.int32, shape, 0) < lax.broadcasted_iota(jnp.int32, shape, 1), 1.0, 0.0).astype(BF)
        slot = lax.broadcasted_iota(jnp.int32, (CAP, TOK), 0).astype(F32)
        q = lax.broadcasted_iota(jnp.int32, (16, TOK), 0)
        step, flip = (q // 2) % SIDE, q // 8
        x, z, c = where[0], where[1], where[2]
        core = jnp.where(flip == 1, 1 - c, c)
        for h in range(2):
            zz = (z + step) % SIDE if h == 0 else z
            xx = x if h == 0 else (x + step) % SIDE
            names = (((xx * SIDE + zz) * 2 + core) * 2 + q % 2).astype(F32)
            for g in range(4):
                ids = metas[h * 4 + g][...].astype(F32)
                match = jnp.zeros((16, TOK), F32)
                for k in range(8):
                    match = match + jnp.where(ids[k:k + 1] == names, 1.0, 0.0)
                place = jnp.where(match > 0.0, dot(match.astype(BF), before), -1.0)
                for n in range(0, 16, 2):
                    two = jnp.concatenate([jnp.where(place[n + e:n + e + 1] == slot, 1.0, 0.0) for e in range(2)], axis=0)
                    p[h * 4 + g, n * CAP:n * CAP + 48, :] = two.astype(BF)

    for h in range(2):
        x0, x1, x2a, x2b, x3 = [r[...] for r in xs[h * 5:h * 5 + 5]]
        dense = [x0, x1, jnp.concatenate([x2a, x2b], axis=0), x3]
        for part in range(2):
            rows = [dot(p[h * 4 + g, part * 192:part * 192 + 192, :], dense[g]) for g in range(4)]
            for n in range(4):
                for e in range(2):
                    at = n * 48 + e * CAP
                    outs[h * 8 + part * 4 + n][e] = jnp.concatenate([r[at:at + CAP] for r in rows], axis=0).astype(BF)


def select(where, near):
    metas = [b for n in near for b in (n[0], n[1], n[2], n[4])]
    return call(select_body, (K // COLS,), [pl.BlockSpec(memory_space=pltpu.SMEM)] + NEAR * 2 + [META] * 8, [ROWS] * 16, [(2, 96, K)] * 16,
                [pltpu.VMEM((8, 384, TOK), BF)])(where, *near[0], *near[1], *metas)


def combine_body(*refs):
    tables, rows, outs = refs[:2], refs[2:18], refs[18:]
    for h in range(2):
        o = outs[h * 7:h * 7 + 7]
        for k in range(2):
            picked = jnp.concatenate([r[e, k * 48:k * 48 + 48, :] for r in rows[h * 8:h * 8 + 8] for e in range(2)], axis=0)
            dense = dot(tables[h][k], picked).astype(BF)
            quarters = [dense[n * 64:n * 64 + 64] for n in range(4)]
            if k == 0:
                o[0][...] = dense[:TOK]
                quarters = quarters[2:]
            for n, part in enumerate(quarters):
                o[(1 if k == 0 else 3) + n][...] = part


def combine(tables, rows):
    shapes = [(TOK, K)] + [(TOK // 2, K)] * 6
    return call(combine_body, (K // COLS,), [PAIRS] * 2 + [ROWS] * 16, ([DENSE] + [PART] * 6) * 2, shapes * 2)(*tables, *rows[0], *rows[1])


def experts_body(y_ref, *refs):
    pieces, (wg, wu, wd), outs = refs[:8], refs[8:11], refs[11:19]
    gu, down, lhs, acc, hs, hid, res, sems, out_sems = refs[19:]
    e = pl.program_id(0)
    y = y_ref[0]

    def stage(k, n):
        if n == 2:
            return [pltpu.make_async_copy(wd.at[k], down.at[k], sems.at[k, 24])]
        copies = []
        for s in range(SIDE):
            copies.append(pltpu.make_async_copy(pieces[n * SIDE + s].at[k], lhs.at[k, n, pl.ds(s * 96, 96), :], sems.at[k, n * 12 + s]))
        for dy in range(SIDE):
            src = pl.ds(pl.multiple_of(lax.rem(y + dy, SIDE) * 1024 + n * F, 128), F)
            dst = pl.ds(n * K + dy * F, F)
            copies.append(pltpu.make_async_copy(wg.at[k, src, :], gu.at[0, k, dst, :], sems.at[k, n * 12 + 4 + dy]))
            copies.append(pltpu.make_async_copy(wu.at[k, src, :], gu.at[1, k, dst, :], sems.at[k, n * 12 + 8 + dy]))
        return copies

    def start(k, n):
        for cp in stage(k, n):
            cp.start()

    def wait(n):
        for cp in stage(e, n):
            cp.wait()

    def results(k, half):
        return [pltpu.make_async_copy(res.at[k, half, pl.ds(s * 96, 96), :], outs[half * SIDE + s].at[k], out_sems.at[k, half * SIDE + s])
                for s in range(SIDE)]

    @pl.when(e == 0)
    def _():
        for k in range(2):
            for n in range(3):
                start(k, n)

    @pl.loop(0, 4)
    def _(n):
        half, kind = n // 2, n % 2
        for k in range(2):
            @pl.when(n == 2 * k)
            def _(k=k):
                wait(k)
        acc[kind, half] = dot(lhs[e, half], gu[kind, e, pl.ds(pl.multiple_of(half * K, K), K), :])

    @pl.loop(0, SIDE * SIDE)
    def _(n):
        to = pl.ds(pl.multiple_of(n * CAP, 8), CAP)
        fro = pl.ds(pl.multiple_of(((n % SIDE) * SIDE + n // SIDE) * CAP, 8), CAP)
        g = acc[0, 1, to, :] + acc[0, 0, fro, :]
        u = acc[1, 1, to, :] + acc[1, 0, fro, :]
        hs[to, :] = g * (1.0 / (1.0 + jnp.exp(-g))) * u

    hid[0] = jnp.concatenate([hs[(j * SIDE + i) * CAP:(j * SIDE + i + 1) * CAP, :] for i in range(SIDE) for j in range(SIDE)], axis=0).astype(BF)
    hid[1] = hs[...].astype(BF)
    wait(2)

    @pl.loop(0, 2 * SIDE)
    def _(n):
        half, dy = n // SIDE, n % SIDE
        src = pl.ds(pl.multiple_of(lax.rem(y + dy, SIDE) * 1024 + half * F, F), F)
        res[e, half, :, pl.ds(pl.multiple_of(dy * F, F), F)] = dot(hid[half], down[e, :, src]).astype(BF)
        for k in range(2):
            @pl.when(n == k * SIDE + SIDE - 1)
            def _(k=k):
                for cp in results(e, k):
                    cp.start()

    @pl.when(e == 1)
    def _():
        for k in range(2):
            for half in range(2):
                for cp in results(k, half):
                    cp.wait()


def experts(y, a, b, wg, wu, wd):
    hbm = pl.BlockSpec(memory_space=pl.ANY)
    scratch = [pltpu.VMEM((2, 2, 2 * K, FF), BF), pltpu.VMEM((2, FF, 2 * K), BF), pltpu.VMEM((2, 2, 384, K), BF),
               pltpu.VMEM((2, 2, 384, FF), F32), pltpu.VMEM((384, FF), F32), pltpu.VMEM((2, 384, FF), BF), pltpu.VMEM((2, 2, 384, K), BF),
               pltpu.SemaphoreType.DMA((2, 25)), pltpu.SemaphoreType.DMA((2, 8))]
    o = call(experts_body, (2,), [pl.BlockSpec(memory_space=pltpu.SMEM)] + [hbm] * 11, [hbm] * 8,
             [(2, 96, K)] * 8, scratch, 44)(y, *a, *b, wg, wu, wd)
    return o[:4], o[4:]


def weighted_table(info, names):
    columns = jnp.stack(info).astype(F32)
    ids, prob = columns[:, :8], columns[:, 8:]
    hit = ids[:, None, :, :] == names[None, :, None, None]
    match = jnp.any(hit, axis=2)
    weight = jnp.sum(jnp.where(hit, prob[:, None, :, :], 0.0), axis=2)
    t = jnp.arange(TOK)
    before = (t[:, None] < t[None, :]).astype(BF)
    place = jnp.einsum("get,tu->geu", match.astype(BF), before, preferred_element_type=F32)
    place = jnp.where(match, place, -1.0).reshape(2, 2, 16, TOK).transpose(0, 2, 1, 3)
    weight = weight.reshape(2, 2, 16, TOK).transpose(0, 2, 1, 3)
    eye = jnp.arange(2)
    same = (eye[:, None] == eye[None, :])[None, None, :, None, :, None]
    on = (place[:, :, None, None, :, :] == jnp.arange(CAP, dtype=F32)[None, None, None, :, None, None]) & same
    wgt = jnp.where(on, weight[:, :, None, None, :, :], 0.0).astype(BF)
    return wgt.reshape(2, 768, 256).swapaxes(1, 2)


def total(terms):
    out = terms[0].astype(F32)
    for t in terms[1:]:
        out = out + t.astype(F32)
    return out


def gather_ring(a, dim):
    half = a.shape[0] // 2
    r1, r3 = recv(a, dim, 1), recv(a, dim, -1)
    return [a, r1, recv(r1[:half], dim, 1), recv(r3[half:], dim, -1), r3]


def scatter_ring(blocks, dim):
    b0, b10, b11, b20, b21, b30, b31 = blocks
    s0, s1 = recv(b20, dim, -1), recv(b21, dim, 1)
    i1, j0 = recv(b11, dim, -1), recv(b30, dim, 1)
    i0 = recv(total([b10, s0]).astype(BF), dim, -1)
    j1 = recv(total([b31, s1]).astype(BF), dim, 1)
    half = b20.shape[0]
    return jnp.concatenate([total([b0[:half], i0, j0]), total([b0[half:], i1, j1])], axis=0)


def body(tokens, expert_ids, gate_prob, gate_weight, up_weight, down_weight):
    ep = lax.axis_index("ep")
    x, z, c = ep // 8, (ep // 2) % SIDE, ep % 2
    where = jnp.stack([x, z, c]).astype(jnp.int32)
    y = lax.axis_index("etp").astype(jnp.int32).reshape(1)
    meta = jnp.concatenate([expert_ids.T.astype(BF), gate_prob.T.astype(BF), jnp.zeros((112, TOK), BF)], axis=0)
    wide = [tokens] + [recv(tokens, "y", d) for d in (1, 2, 3)]
    axes = (("x", "z"), ("z", "x"))
    near = [gather_ring(jnp.concatenate([w[:, h * F:(h + 1) * F] for w in wide] + [meta], axis=1), dim)
            for h, (dim, far) in enumerate(axes)]
    picked = select(where, near)
    rows, got, tables = [{}, {}], [{}, {}], []
    for h, (dim, far) in enumerate(axes):
        mates = []
        for s, dc in PIECES:
            mate = ep_of(x, z + s, c ^ dc) if far == "z" else ep_of(x + s, z, c ^ dc)
            mates += [2 * mate, 2 * mate + 1]
            out = picked[h * 8 + PIECES.index(((-s) % SIDE, dc))]
            rows[h][s, dc] = out if (s, dc) == (0, 0) else recv(out, far, s, dc)
        n = near[h]
        tables.append(weighted_table([m[:16, K:] for m in (n[0], n[1], n[2], n[4])], jnp.stack(mates).astype(F32)))
    for dc in range(2):
        outs = experts(y, *[[rows[h][s, dc] for s in range(SIDE)] for h in range(2)], gate_weight, up_weight, down_weight)
        for h, (dim, far) in enumerate(axes):
            for s in range(SIDE):
                out = outs[h][(-s) % SIDE]
                got[h][s, dc] = out if (s, dc) == (0, 0) else recv(out, far, s, dc)
    dense = combine(tables, [[got[h][q] for q in PIECES] for h in range(2)])
    halves = [scatter_ring(dense[h * 7:h * 7 + 7], dim).astype(BF) for h, (dim, far) in enumerate(axes)]
    parts = [jnp.concatenate([halves[h][:, d * F:(d + 1) * F] for h in range(2)], axis=1) for d in range(SIDE)]
    return total([parts[0]] + [recv(parts[d], "y", -d) for d in (1, 2, 3)]).astype(BF)


def solution(mesh):
    in_specs = (P("ep", "etp"), P("ep", None), P("ep", None), P("ep", None, "etp"), P("ep", None, "etp"), P("ep", "etp", None))

    return jax.shard_map(body, mesh=mesh, in_specs=in_specs, out_specs=P("ep", "etp"), check_vma=False)
```
